256 devices in a mesh: rows: 32 (over y, x, core), rhs: 8 (over z).
Axes of the slice: x: 4, y: 4, z: 8, core: 2. Of those that a mesh axis runs over, the one named last changes fastest.
Arguments:
- sources: bfloat16 [131072, 4096], P('rows', 'rhs'), may hold values from -6 to 6
- near_blocks: bfloat16 [512, 3, 256, 256], P('rows'), may hold values from -0.21875 to 0.21875
- near_list: int32 [512, 3], P('rows'), may hold values from 0 to 511, as said below
- source_basis: bfloat16 [512, 256, 32], P('rows'), may hold values from -0.375 to 0.375
- target_basis: bfloat16 [512, 256, 32], P('rows'), may hold values from -0.375 to 0.375
- transfer_fine: bfloat16 [896, 32, 32], P('rows'), may hold values from -0.875 to 0.875
- transfer_coarse: bfloat16 [128, 32, 32], P('rhs'), may hold values from -0.875 to 0.875
- couple_fine: bfloat16 [896, 3, 32, 32], P('rows'), may hold values from -0.625 to 0.625
- couple_coarse: bfloat16 [128, 3, 32, 32], P('rhs'), may hold values from -0.625 to 0.625
- far_fine: int32 [896, 3], P('rows'), may hold values from 0 to 511, as said below
- far_coarse: int32 [128, 3], replicated, may hold values from -1 to 63, as said below
Outputs:
- potentials: bfloat16 [131072, 4096], P('rows', 'rhs')
The draws below stay inside these ranges and needn't reach their ends.
Inputs may be any that keep to these rules, and one draw needn't show every extreme that they name: `near_list`: row t lists the leaf clusters t - 1, t and t + 1 modulo 512 in some order. `far_fine`: row d * 28 + o + i belongs to cluster d * m + i of the level with n = m * 32 clusters, where (o, m) is (0, 16), (16, 8) or (24, 4). It lists, in some order, the three clusters of that level that are children of the cyclic neighbours of the cluster's parent and not cyclic neighbours of the cluster: for cluster j with parent p = j // 2, the clusters 2p - 2, 2p + 2, 2p + 3 if j is even and 2p - 2, 2p - 1, 2p + 3 if j is odd, modulo n. `far_coarse`: row n + j for n = 8, 16, ..., 64 lists, in some order, the three far clusters of cluster j of the level with n clusters by the rule of far_fine. Row 4 + j holds (j + 2) modulo 4 in slot 0 and -1 in slots 1 and 2. Rows 0 to 3 hold -1.
All inputs are finite; a program needn't handle non-finite values.
Results may differ from the reference program's by a relative error of at most 0.012.
Values may be sent and summed in bfloat16 or wider, within the bound.
A program may use at most 128 MiB of HBM per device.

```python
import jax
import jax.numpy as jnp
from jax import lax

LEAF = 256
RANK = 32
LPD = 16
LEAVES = 512
POINTS = 131072
RHS = 4096
FINE = 896
COARSE = 128


def shuffle_rows(key, table):
    keys = jax.random.split(key, table.shape[0])

    def one_order(single):
        return jax.random.permutation(single, 3)
    orders = jax.vmap(one_order)(keys)
    return jnp.take_along_axis(table, orders, axis=1)


def far_rule(index, clusters):
    parent = index // 2
    second = jnp.where(index % 2 == 1, 2 * parent - 1, 2 * parent + 2)
    first = (2 * parent - 2 + 4 * clusters) % clusters
    second = (second + 4 * clusters) % clusters
    third = (2 * parent + 3) % clusters
    return jnp.stack([first, second, third], axis=1).astype(jnp.int32)


def draw_near_list(key, part):
    leaves = jnp.arange(LEAVES, dtype=jnp.int32)
    table = jnp.stack([(leaves + LEAVES - 1) % LEAVES, leaves, (leaves + 1) % LEAVES], axis=1)
    return shuffle_rows(jax.random.fold_in(key, 11), table)


def draw_far_fine(key, part):
    row_count = LEAVES // LPD
    block = LPD + LPD // 2 + LPD // 4
    rows_all = jnp.arange(row_count * block, dtype=jnp.int32)
    device = rows_all // block
    within = rows_all % block
    local_count = jnp.where(within < LPD, LPD, jnp.where(within < LPD + LPD // 2, LPD // 2, LPD // 4))
    offset = jnp.where(within < LPD, 0, jnp.where(within < LPD + LPD // 2, LPD, LPD + LPD // 2))
    index = device * local_count + within - offset
    table = far_rule(index, local_count * row_count)
    return shuffle_rows(jax.random.fold_in(key, 23), table)


def draw_far_coarse(key, part):
    row_count = LEAVES // LPD
    empty = jnp.full((4,), -1, jnp.int32)
    top = jnp.arange(4, dtype=jnp.int32)
    pieces = [jnp.full((4, 3), -1, jnp.int32), jnp.stack([(top + 2) % 4, empty, empty], axis=1)]
    clusters = 8
    for level in range((2 * row_count).bit_length() - 3):
        index = jnp.arange(clusters, dtype=jnp.int32)
        pieces.append(shuffle_rows(jax.random.fold_in(key, 100 + clusters), far_rule(index, clusters)))
        clusters = clusters * 2
    return jnp.concatenate(pieces, axis=0)


def block_scale(own_key, dims, cuts, low, largest):
    def one(position, parts):
        heights = jax.random.uniform(jax.random.fold_in(jax.random.fold_in(own_key, 6), position), (parts,), jnp.float32, low / len(cuts), largest / len(cuts))
        return jnp.repeat(jnp.exp(heights), dims[position] // parts).reshape((-1,) + (1,) * (len(dims) - position - 1))

    gain = one(*cuts[0])
    for cut in cuts[1:]:
        gain = gain * one(*cut)
    return gain


def centred(stream_key, extent, deviation, most, shards=(), held_as=jnp.bfloat16):
    gain = block_scale(stream_key, extent, shards, -0.22, 0.18) if shards else 1.0
    values = jax.random.normal(stream_key, extent, jnp.float32) * deviation * gain
    return jnp.minimum(jnp.maximum(values, -most), most).astype(held_as)


def setup_inputs(seed: int = 0) -> dict:
    splits = jax.random.split(jax.random.key(seed), 12)
    sources = centred(splits[0], (POINTS, RHS), 1.0, 6.0, ((0, 32), (1, 8)))
    near_blocks = centred(splits[1], (LEAVES, 3, LEAF, LEAF), (3 * LEAF) ** -0.5, 0.21875, ((0, 32),))
    near_list = draw_near_list(jax.random.fold_in(splits[11], 71), 0)
    source_basis = centred(splits[3], (LEAVES, LEAF, RANK), LEAF ** -0.5, 0.375, ((0, 32),))
    target_basis = centred(splits[4], (LEAVES, LEAF, RANK), (8 * RANK) ** -0.5, 0.375, ((0, 32),))
    transfer_fine = centred(splits[5], (FINE, RANK, RANK), (3 * RANK // 2) ** -0.5, 0.875, ((0, 32),))
    transfer_coarse = centred(splits[6], (COARSE, RANK, RANK), (3 * RANK // 2) ** -0.5, 0.875, ((0, 8),))
    couple_fine = centred(splits[7], (FINE, 3, RANK, RANK), (3 * RANK) ** -0.5, 0.625, ((0, 32),))
    couple_coarse = centred(splits[8], (COARSE, 3, RANK, RANK), (3 * RANK) ** -0.5, 0.625, ((0, 8),))
    far_fine = draw_far_fine(jax.random.fold_in(splits[11], 71), 0)
    far_coarse = draw_far_coarse(jax.random.fold_in(splits[11], 71), 0)
    return dict(sources=sources, near_blocks=near_blocks, near_list=near_list, source_basis=source_basis, target_basis=target_basis, transfer_fine=transfer_fine, transfer_coarse=transfer_coarse, couple_fine=couple_fine, couple_coarse=couple_coarse, far_fine=far_fine, far_coarse=far_coarse)


def fine_level(table, row_count, first, count):
    block = table.shape[0] // row_count
    shaped = table.reshape((row_count, block) + table.shape[1:])
    return shaped[:, first:first + count].reshape((row_count * count,) + table.shape[1:])


def couple(moments, blocks, partners):
    valid = partners >= 0
    picked = moments[jnp.maximum(partners, 0)]
    picked = jnp.where(valid[:, :, None, None], picked, jnp.zeros_like(picked))
    return jnp.einsum('nsab,nsbr->nar', blocks.astype(jnp.float32), picked.astype(jnp.float32))


def lift(moments, transfer):
    clusters, rank, width = moments.shape
    product = jnp.einsum('nab,nar->nbr', transfer.astype(jnp.float32), moments.astype(jnp.float32))
    return product.reshape(clusters // 2, 2, rank, width).sum(axis=1).astype(jnp.bfloat16)


def lower(parent, transfer, coupled):
    spread = jnp.repeat(parent, 2, axis=0)
    carried = jnp.einsum('nab,nbr->nar', transfer.astype(jnp.float32), spread.astype(jnp.float32))
    return (coupled + carried).astype(jnp.bfloat16)


def reference(sources, near_blocks, near_list, source_basis, target_basis, transfer_fine, transfer_coarse, couple_fine, couple_coarse, far_fine, far_coarse):
    row_count = LEAVES // LPD
    width = sources.shape[1]
    counts = [LPD, LPD // 2, LPD // 4]
    firsts = [0, LPD, LPD + LPD // 2]
    shaped = sources.reshape(LEAVES, LEAF, width)

    def leaf_moments(index):
        return jnp.dot(source_basis[index].T, shaped[index], preferred_element_type=jnp.float32).astype(jnp.bfloat16)

    moments = lax.map(leaf_moments, jnp.arange(LEAVES, dtype=jnp.int32))
    upward = [moments]
    fine_tables = []
    for level in range(3):
        transfer = fine_level(transfer_fine, row_count, firsts[level], counts[level])
        blocks = fine_level(couple_fine, row_count, firsts[level], counts[level])
        partners = fine_level(far_fine, row_count, firsts[level], counts[level])
        fine_tables.append((transfer, blocks, partners))
        moments = lift(moments, transfer)
        upward.append(moments)
    clusters = 2 * row_count
    depth = clusters.bit_length() - 3
    coarse_up = [moments]
    for step in range(depth):
        moments = lift(moments, transfer_coarse[clusters:2 * clusters])
        clusters = clusters // 2
        coarse_up.append(moments)
    downward = moments
    for step in range(depth + 1):
        coupled = couple(coarse_up[depth - step], couple_coarse[clusters:2 * clusters], far_coarse[clusters:2 * clusters])
        if step == 0:
            downward = coupled.astype(jnp.bfloat16)
        else:
            downward = lower(downward, transfer_coarse[clusters:2 * clusters], coupled)
        clusters = clusters * 2
    for level in (2, 1, 0):
        transfer, blocks, partners = fine_tables[level]
        coupled = couple(upward[level], blocks, partners)
        downward = lower(downward, transfer, coupled)

    def leaf_output(index):
        summed = jnp.dot(target_basis[index], downward[index], preferred_element_type=jnp.float32)
        for slot in range(3):
            summed = summed + jnp.dot(near_blocks[index, slot], shaped[near_list[index, slot]], preferred_element_type=jnp.float32)
        return summed.astype(jnp.bfloat16)

    result = lax.map(leaf_output, jnp.arange(LEAVES, dtype=jnp.int32))
    return result.reshape(LEAVES * LEAF, width)
```

```python
import jax
import jax.numpy as jnp
from jax import lax
from jax.experimental import pallas as pl
from jax.experimental.pallas import tpu as pltpu
from jax.sharding import PartitionSpec as P

MESH = pl.DeviceIdType.MESH
BF = jnp.bfloat16
F32 = jnp.float32
LEAF, RANK, LPD = 256, 32, 16
ROWS, CHIPS, DEEP = 32, 16, 8
WIDE, HALF = 512, 256
NEAR_FIRST = 8


def dot(a, b):
    return jnp.dot(a, b, preferred_element_type=F32)


def dot_t(a, b):
    return lax.dot_general(a, b, (((0,), (0,)), ((), ())), preferred_element_type=F32)


def dot_nt(a, b):
    return lax.dot_general(a, b, (((1,), (1,)), ((), ())), preferred_element_type=F32)


def iota(shape, dim):
    return lax.broadcasted_iota(jnp.int32, shape, dim)


def block_mask(shape, row_div, lane_div):
    return (iota(shape, 0) // row_div) % 4 == (iota(shape, 1) // lane_div) % 4


def routed(spread, fars, base, size):
    lanes = iota((RANK, 128), 1) // RANK
    total = jnp.zeros((RANK, 128), F32)
    for slot in range(3):
        place = (fars[slot] - base) & (size - 1)
        place = jnp.where(place < 2, place, place - 2)
        total = total + jnp.where(lanes == place, spread[slot * RANK : (slot + 1) * RANK], 0.0)
    return total


def tree_kernel(
    near_list, far_fine, far_coarse,
    sources, near_blocks, basis, transfer_fine, couple_fine, transfer_coarse, couple_coarse,
    moments_out, near_out,
    near, xs, nb, sb, tf, cf, tc, cc,
    eb, eu, s4, c512, c256, c128, c64, n64, n32, c16, c8, c4, f64,
    g512, g256, g128, g64, g32,
    se, ss, re64, re32, re16, re8, rs64, rs32, rs16, rs8, rs4,
    load_sem, store_sem, tab_send, tab_recv, halo_send, halo_recv, ring_send, ring_recv,
):
    r = lax.axis_index("rows")
    z = lax.axis_index("rhs")
    k = r // 2
    c = r % 2
    left, right = (r + ROWS - 1) % ROWS, (r + 1) % ROWS
    left2, right2 = (r + ROWS - 2) % ROWS, (r + 2) % ROWS
    partner = r + 1 - 2 * c
    other = (r + ROWS + 2 * c - 1) % ROWS
    z32, z64 = 2 + k // 8, 4 + k // 4

    barrier = pltpu.get_barrier_semaphore()

    def greet_rows(d, carry):
        there = ((k + d) % CHIPS) * 2 + c
        pl.semaphore_signal(barrier, inc=1, device_id={"rows": there}, device_id_type=MESH)
        return carry

    def greet_deep(d, carry):
        pl.semaphore_signal(barrier, inc=1, device_id={"rhs": (z + d) % DEEP}, device_id_type=MESH)
        return carry

    lax.fori_loop(1, DEEP, greet_deep, 0)
    lax.fori_loop(1, CHIPS, greet_rows, 0)
    for there in (partner, other):
        pl.semaphore_signal(barrier, inc=1, device_id={"rows": there}, device_id_type=MESH)

    loads = []

    def load(src, dst):
        copy = pltpu.make_async_copy(src, dst, load_sem.at[len(loads)])
        copy.start()
        loads.append(copy)
        return copy

    get_tc = load(transfer_coarse, tc)
    get_cc = load(couple_coarse, cc)
    get_tf = load(transfer_fine, tf)
    get_sb = load(basis, sb)
    chunk = 4 * LEAF
    get_xs = [
        load(sources.at[pl.ds(i * chunk, chunk)], xs.at[pl.ds(LEAF + i * chunk, chunk)]) for i in range(4)
    ]
    get_cf = load(couple_fine, cf)
    get_nb = load(near_blocks, nb)

    spread = jnp.where(iota((RANK, 128), 1) % RANK == iota((RANK, 128), 0), 1.0, 0.0).astype(BF)
    spread_t = jnp.where(iota((128, RANK), 0) % RANK == iota((128, RANK), 1), 1.0, 0.0).astype(BF)

    get_tc.wait()
    wide_e = dot(tc[...].reshape(LPD * RANK, RANK), spread)
    lane_block = iota((RANK, 128), 1) // RANK
    for group in range(2):
        for odd in range(2):
            total = jnp.zeros((RANK, 128), F32)
            for parent in range(4):
                row = (8 * group + 2 * parent + odd) * RANK
                total = total + jnp.where(lane_block == parent, wide_e[row : row + RANK], 0.0)
            se[group, odd * RANK : (odd + 1) * RANK, :] = total.astype(BF)
    get_cc.wait()
    for quarter in range(4):
        wide_s = dot(cc[4 * quarter : 4 * quarter + 4].reshape(4 * 3 * RANK, RANK), spread)
        first_size = {0: 4, 1: 4, 2: 8, 3: 8}[quarter]
        size = jnp.where(z >= 4, 64, jnp.where(z >= 2, 32, jnp.where(z == 1, 16, first_size)))
        for i in range(4):
            row = 4 * quarter + i
            mine = wide_s[i * 3 * RANK : (i + 1) * 3 * RANK]
            heap = z * LPD + row
            at = heap - size
            base = at - row % 2 - 2
            fars = [far_coarse[slot, heap] for slot in range(3)]
            block = routed(mine, fars, base, size)
            if quarter == 1:
                block = jnp.where(z == 0, mine[:RANK], block)
            ss[row * RANK : (row + 1) * RANK, :] = block.astype(BF)

    get_tf.wait()
    fine_e = tf[...].reshape(28 * RANK, RANK)
    eb[...] = jnp.where(block_mask((896, 128), 64, RANK), dot(fine_e, spread), 0.0).astype(BF)
    eu[...] = jnp.where(block_mask((128, 896), RANK, 64), dot_nt(spread_t, fine_e), 0.0).astype(BF)

    get_sb.wait()
    for i in range(4):
        get_xs[i].wait()
        for leaf in range(4 * i, 4 * i + 4):
            product = dot(sb[leaf], xs[LEAF * (leaf + 1) : LEAF * (leaf + 2), :])
            c512[64 + RANK * leaf : 64 + RANK * (leaf + 1), :] = product.astype(BF)

    pl.semaphore_wait(barrier, DEEP - 1 + CHIPS - 1 + 2)

    def table_copy(kind, src, dst, slot, d):
        return pltpu.make_async_remote_copy(
            src_ref=src, dst_ref=dst, send_sem=tab_send.at[slot, d], recv_sem=tab_recv.at[kind],
            device_id={"rhs": (z + d) % DEEP}, device_id_type=MESH,
        )

    e64_at = se.at[(k % 4) // 2]
    e32_at = se.at[(k % 8) // 4]
    rows64 = pl.ds(((4 * k) % LPD) * RANK, 4 * RANK)
    rows32 = pl.ds(((2 * k) % LPD) * RANK, 2 * RANK)
    rows16 = pl.ds(k * RANK, RANK)
    rows8 = pl.ds((8 + k // 2) * RANK, RANK)
    rows4 = pl.ds((4 + k // 4) * RANK, RANK)
    tables = [
        (z64, [(0, e64_at, re64), (1, ss.at[rows64], rs64)]),
        (z32, [(2, e32_at, re32), (3, ss.at[rows32], rs32)]),
        (1, [(4, se, re16), (5, ss.at[rows16], rs16)]),
        (0, [(6, se.at[1], re8), (7, ss.at[rows8], rs8), (8, ss.at[rows4], rs4)]),
    ]
    for owner, items in tables:
        @pl.when(z == owner)
        def _(items=items):
            for slot, (kind, src, dst) in enumerate(items):
                def send(d, carry, kind=kind, src=src, dst=dst, slot=slot):
                    table_copy(kind, src, dst, slot, d).start()
                    return carry
                lax.fori_loop(1, DEEP, send, 0)
                dst[...] = src[...]

    def wait_table(index, item):
        owner, items = tables[index]
        kind, src, dst = items[item]

        @pl.when(z != owner)
        def _():
            table_copy(kind, src, dst, item, 1).wait_recv()

    halos = []

    def swap(src, dst, there):
        index = len(halos)
        copy = pltpu.make_async_remote_copy(
            src_ref=src, dst_ref=dst, send_sem=halo_send.at[index], recv_sem=halo_recv.at[index],
            device_id={"rows": there}, device_id_type=MESH,
        )
        copy.start()
        halos.append(copy)
        return copy

    own = c512[64:576, :]
    c256[64:192, :] = dot(eu[:, 0:256], own[:256]).astype(BF)
    c256[192:320, :] = dot(eu[:, 256:512], own[256:]).astype(BF)
    c128[64:192, :] = dot(eu[:, 512:768], c256[64:320, :]).astype(BF)
    mine64 = dot(eu[:64, 768:896], c128[64:192, :]).astype(BF)
    c64[0] = mine64[:, :HALF]
    c64[1] = mine64[:, HALF:]
    rows_mine = pl.ds(64 + 64 * c, 64)
    rows_theirs = pl.ds(128 - 64 * c, 64)
    to_partner = swap(c64.at[1 - c], n64.at[rows_mine], partner)
    n64[rows_mine, :] = c64[c]

    leaf_left = swap(xs.at[pl.ds(LEAF, LEAF)], xs.at[pl.ds(17 * LEAF, LEAF)], left)
    leaf_right = swap(xs.at[pl.ds(16 * LEAF, LEAF)], xs.at[pl.ds(0, LEAF)], right)
    level_halos = []
    for held, count in ((c128, 4), (c256, 8), (c512, 16)):
        rows = count * RANK
        level_halos.append((
            swap(held.at[pl.ds(64, 64)], held.at[pl.ds(64 + rows, 64)], left),
            swap(held.at[pl.ds(rows, 64)], held.at[pl.ds(0, 64)], right),
        ))

    get_nb.wait()

    def near_leaf(t, carry):
        blocks = []
        for wanted in (-1, 0, 1):
            target = (r * LPD + t + wanted) & 511
            slot = jnp.where(near_list[2, t] == target, 2, jnp.where(near_list[1, t] == target, 1, 0))
            blocks.append(nb[t, slot])
        rows = xs[pl.ds(pl.multiple_of(t * LEAF, LEAF), 3 * LEAF), :]
        near[pl.ds(pl.multiple_of(t * LEAF, LEAF), LEAF), :] = dot(jnp.concatenate(blocks, axis=1), rows).astype(BF)
        return carry

    lax.fori_loop(1, 1 + NEAR_FIRST, near_leaf, 0)
    stores = []

    def store(first, count):
        rows = pl.ds(first * LEAF, count * LEAF)
        copy = pltpu.make_async_copy(near.at[rows], near_out.at[rows], store_sem.at[len(stores)])
        copy.start()
        stores.append(copy)

    to_partner.wait_recv()
    wait_table(0, 0)
    children = iota((128, 128), 0) // RANK
    lanes = iota((128, 128), 1) // RANK
    packed = re64[...].astype(F32)
    eb64 = jnp.where(lanes == 2 * (k % 2) + children // 2, jnp.concatenate([packed, packed], axis=0), 0.0).astype(BF)
    up = dot_t(eb64, n64[64:192, :])
    n32[64:128, :] = (up[:64] + up[64:]).astype(BF)
    wait_table(1, 0)
    eb32 = jnp.where(iota((64, 128), 1) // RANK == k % 4, re32[...].astype(F32), 0.0).astype(BF)
    up = dot_t(eb32, n32[64:128, :])
    c16[k] = (up[:32] + up[32:64] + up[64:96] + up[96:]).astype(BF)

    def ring_copy(src_chip, there, d):
        return pltpu.make_async_remote_copy(
            src_ref=c16.at[src_chip], dst_ref=c16.at[src_chip],
            send_sem=ring_send.at[d], recv_sem=ring_recv.at[src_chip],
            device_id={"rows": there * 2 + c}, device_id_type=MESH,
        )

    def ring_start(d, carry):
        ring_copy(k, (k + d) % CHIPS, d).start()
        return carry

    lax.fori_loop(1, CHIPS, ring_start, 0)
    halos64 = (
        swap(n64.at[pl.ds(64, 64)], n64.at[pl.ds(192, 64)], left2),
        swap(n64.at[pl.ds(128, 64)], n64.at[pl.ds(0, 64)], right2),
    )
    halos32 = (
        swap(n32.at[pl.ds(64, 64)], n32.at[pl.ds(128, 64)], left2),
        swap(n32.at[pl.ds(64, 64)], n32.at[pl.ds(0, 64)], right2),
    )

    get_cf.wait()
    for part in range(7):
        wide_s = dot(cf[4 * part : 4 * part + 4].reshape(4 * 3 * RANK, RANK), spread)
        size, first = ((512, 0), (256, 16), (128, 24))[0 if part < 4 else 1 if part < 6 else 2]
        for i in range(4):
            row = 4 * part + i
            j = r * (size // ROWS) + row - first
            fars = [far_fine[slot, row] for slot in range(3)]
            block = routed(wide_s[i * 3 * RANK : (i + 1) * 3 * RANK], fars, j - row % 2 - 2, size)
            s4[row * RANK : (row + 1) * RANK, :] = block.astype(BF)

    for (from_left, from_right), held, count, first, out in (
        (level_halos[0], c128, 4, 24, g128), (level_halos[1], c256, 8, 16, g256), (level_halos[2], c512, 16, 0, g512),
    ):
        from_left.wait_recv()
        from_right.wait_recv()
        for pair in range(count // 2):
            window = jnp.concatenate([held[64 * pair : 64 * pair + 64, :], held[64 * pair + 128 : 64 * pair + 192, :]], axis=0)
            blocks = s4[first * RANK + 64 * pair : first * RANK + 64 * pair + 64, :]
            out[64 * pair : 64 * pair + 64, :] = dot(blocks, window)

    store(1, NEAR_FIRST)
    lax.fori_loop(1 + NEAR_FIRST, 15, near_leaf, 0)
    leaf_left.wait_recv()
    leaf_right.wait_recv()
    near_leaf(0, 0)
    near_leaf(15, 0)
    store(1 + NEAR_FIRST, 14 - NEAR_FIRST)

    for copies, held, table, blocks, out, pairs in (
        (halos64, n64, 0, rs64, g64, 2), (halos32, n32, 1, rs32, g32, 1),
    ):
        for copy in copies:
            copy.wait_recv()
        wait_table(table, 1)
        for pair in range(pairs):
            window = jnp.concatenate([held[64 * pair : 64 * pair + 64, :], held[64 * pair + 128 : 64 * pair + 192, :]], axis=0)
            out[64 * pair : 64 * pair + 64, :] = dot(blocks[64 * pair : 64 * pair + 64, :], window)

    store(0, 1)
    store(15, 1)

    for item in range(2):
        wait_table(2, item)
    for item in range(3):
        wait_table(3, item)
    mask8 = iota((256, 128), 1) // RANK == iota((256, 128), 0) // 64
    def eight(block):
        wide = block.astype(F32)
        return jnp.where(mask8, jnp.concatenate([wide] * 4, axis=0), 0.0).astype(BF)

    def own_child(block, odd, parent):
        even_rows, odd_rows = block[:RANK].astype(F32), block[RANK:].astype(F32)
        rows = jnp.where(odd == 1, odd_rows, even_rows)
        return jnp.where(iota((RANK, 128), 1) // RANK == parent, rows, 0.0).astype(BF)

    e16 = [eight(re16[0]), eight(re16[1])]
    e8 = eight(re8[...])
    e16_own = own_child(re16[k // 8], k % 2, (k % 8) // 2)
    e8_own = own_child(re8[...], (k // 2) % 2, k // 4)

    def ring_wait(d, carry):
        ring_copy((k + d) % CHIPS, k, d).wait_recv()
        return carry

    lax.fori_loop(1, CHIPS, ring_wait, 0)
    p16 = k // 2
    for group in range(2):
        up = dot_t(e16[group], c16[8 * group : 8 * group + 8].reshape(256, HALF)).astype(BF)
        c8[2 * group] = up[:64]
        c8[2 * group + 1] = up[64:]
    p8 = k // 4
    all8 = c8[...].reshape(256, HALF)
    up = dot_t(e8, all8).astype(BF)
    for j in range(4):
        c4[j] = up[RANK * j : RANK * (j + 1)]
    window = jnp.concatenate(
        [c16[pl.ds(2 * ((p16 + 7) % 8), 2)].reshape(64, HALF), c16[pl.ds(2 * ((p16 + 1) % 8), 2)].reshape(64, HALF)], axis=0
    )
    g16 = dot(rs16[...], window)
    g8 = dot(rs8[...], jnp.concatenate([c8[(p8 + 3) % 4], c8[(p8 + 1) % 4]], axis=0))
    f4 = dot(rs4[:, :RANK], c4[(k // 4 + 2) % 4]).astype(BF)
    f8 = (g8 + dot(e8_own, jnp.concatenate([f4] * 4, axis=0))).astype(BF)
    f16 = (g16 + dot(e16_own, jnp.concatenate([f8] * 4, axis=0))).astype(BF)

    f32_ = (g32[...] + dot(eb32, jnp.concatenate([f16] * 4, axis=0))).astype(BF)
    f64_ = (g64[...] + dot(eb64, jnp.concatenate([f32_] * 2, axis=0))).astype(BF)
    f64[0] = f64_[:64]
    f64[1] = f64_[64:]
    back = swap(f64.at[1 - c], f64.at[2 + c], partner)
    f64[2 + c] = f64[c]
    back.wait_recv()
    parents = jnp.concatenate([f64[2], f64[3]], axis=1)
    f128 = (g128[...] + dot(eb[768:896, :64], parents)).astype(BF)
    f256 = (g256[...] + dot(eb[512:768, :], f128)).astype(BF)
    for group in range(2):
        rows = slice(256 * group, 256 * group + 256)
        moments_out[rows, :] = (g512[rows, :] + dot(eb[rows, :], f256[128 * group : 128 * group + 128])).astype(BF)

    for copy in halos:
        copy.wait_send()
    for copy in stores:
        copy.wait()

    def ring_sent(d, carry):
        ring_copy(k, (k + d) % CHIPS, d).wait_send()
        return carry

    lax.fori_loop(1, CHIPS, ring_sent, 0)
    for owner, items in tables:
        @pl.when(z == owner)
        def _(items=items):
            for slot, (kind, src, dst) in enumerate(items):
                def sent(d, carry, kind=kind, src=src, dst=dst, slot=slot):
                    table_copy(kind, src, dst, slot, d).wait_send()
                    return carry
                lax.fori_loop(1, DEEP, sent, 0)


def tree(near_list, far_fine, far_coarse, sources, near_blocks, basis, transfer_fine, couple_fine, transfer_coarse, couple_coarse):
    smem = pl.BlockSpec(memory_space=pltpu.SMEM)
    hbm = pl.BlockSpec(memory_space=pl.ANY)
    vmem = pl.BlockSpec(memory_space=pltpu.VMEM)
    V = pltpu.VMEM
    dma = pltpu.SemaphoreType.DMA
    scratch = [
        V((4096, WIDE), BF),
        V((18 * LEAF, WIDE), BF), V((16, 3, LEAF, LEAF), BF), V((16, RANK, LEAF), BF), V((28, RANK, RANK), BF),
        V((28, 3, RANK, RANK), BF), V((16, RANK, RANK), BF), V((16, 3, RANK, RANK), BF),
        V((896, 128), BF), V((128, 896), BF), V((896, 128), BF),
        V((640, WIDE), BF), V((384, WIDE), BF), V((256, WIDE), BF), V((2, 64, HALF), BF),
        V((256, HALF), BF), V((192, HALF), BF), V((16, RANK, HALF), BF), V((4, 64, HALF), BF), V((4, RANK, HALF), BF),
        V((4, 64, HALF), BF),
        V((512, WIDE), F32), V((256, WIDE), F32), V((128, WIDE), F32), V((128, HALF), F32), V((64, HALF), F32),
        V((2, 64, 128), BF), V((512, 128), BF), V((64, 128), BF), V((64, 128), BF), V((2, 64, 128), BF), V((64, 128), BF),
        V((128, 128), BF), V((64, 128), BF), V((32, 128), BF), V((32, 128), BF), V((32, 128), BF),
        dma((10,)), dma((4,)), dma((3, DEEP)), dma((9,)), dma((14,)), dma((14,)), dma((CHIPS,)), dma((CHIPS,)),
    ]
    return pl.pallas_call(
        tree_kernel,
        name="tree",
        out_shape=(jax.ShapeDtypeStruct((512, WIDE), BF), jax.ShapeDtypeStruct((4096, WIDE), BF)),
        in_specs=[smem] * 3 + [hbm] * 7,
        out_specs=(vmem, hbm),
        scratch_shapes=scratch,
        compiler_params=pltpu.CompilerParams(
            collective_id=0, has_side_effects=True, vmem_limit_bytes=67043328
        ),
    )(near_list, far_fine, far_coarse, sources, near_blocks, basis, transfer_fine, couple_fine, transfer_coarse, couple_coarse)


def join_kernel(near, basis, moments, out):
    for i in range(2):
        rows = slice(LEAF * i, LEAF * (i + 1))
        far = dot_t(basis[i], moments[RANK * i : RANK * (i + 1), :])
        out[rows, :] = (near[rows, :].astype(F32) + far).astype(BF)


def join(near, basis, moments):
    return pl.pallas_call(
        join_kernel,
        name="join",
        grid=(8,),
        out_shape=jax.ShapeDtypeStruct((4096, WIDE), BF),
        in_specs=[
            pl.BlockSpec((512, WIDE), lambda i: (i, 0)),
            pl.BlockSpec((2, RANK, LEAF), lambda i: (i, 0, 0)),
            pl.BlockSpec((64, WIDE), lambda i: (i, 0)),
        ],
        out_specs=pl.BlockSpec((512, WIDE), lambda i: (i, 0)),
    )(near, basis, moments)


def body(
    sources, near_blocks, near_list, source_basis, target_basis, transfer_fine, transfer_coarse,
    couple_fine, couple_coarse, far_fine, far_coarse,
):
    moments, near = tree(
        near_list.T, far_fine.T, far_coarse.T, sources, near_blocks, jnp.swapaxes(source_basis, 1, 2),
        transfer_fine, couple_fine, transfer_coarse, couple_coarse,
    )
    return join(near, jnp.swapaxes(target_basis, 1, 2), moments)


def solution(mesh):
    in_specs = (
        P("rows", "rhs"), P("rows", None, None, None), P("rows", None), P("rows", None, None), P("rows", None, None),
        P("rows", None, None), P("rhs", None, None), P("rows", None, None, None), P("rhs", None, None, None),
        P("rows", None), P(),
    )
    return jax.shard_map(body, mesh=mesh, in_specs=in_specs, out_specs=P("rows", "rhs"), check_vma=False)
```

```python
import jax
import jax.numpy as jnp
from jax import lax
from jax.experimental import pallas as pl
from jax.experimental.pallas import tpu as pltpu
from jax.sharding import PartitionSpec as P

MESH = pl.DeviceIdType.MESH
BF = jnp.bfloat16
F32 = jnp.float32
LEAF, RANK, LPD = 256, 32, 16
ROWS, CHIPS, DEEP = 32, 16, 8
WIDE, HALF = 512, 256
UNROLL, NEAR_A, NEAR_B = 2, 2, 8
TREE_VMEM = 50_000_000


def dot(a, b):
    return jnp.dot(a, b, preferred_element_type=F32)


def dot_t(a, b):
    return lax.dot_general(a, b, (((0,), (0,)), ((), ())), preferred_element_type=F32)


def dot_nt(a, b):
    return lax.dot_general(a, b, (((1,), (1,)), ((), ())), preferred_element_type=F32)


def iota(shape, dim):
    return lax.broadcasted_iota(jnp.int32, shape, dim)


def block_mask(shape, row_div, lane_div):
    return (iota(shape, 0) // row_div) % 4 == (iota(shape, 1) // lane_div) % 4


def routed(spread, fars, base, size):
    lanes = iota((RANK, 128), 1) // RANK
    total = jnp.zeros((RANK, 128), F32)
    for slot in range(3):
        place = (fars[slot] - base) & (size - 1)
        place = jnp.where(place < 2, place, place - 2)
        total = total + jnp.where(lanes == place, spread[slot * RANK : (slot + 1) * RANK], 0.0)
    return total


def tree_kernel(
    near_list_in, far_fine_in, far_coarse_in,
    sources, near_blocks, basis, transfer_fine, couple_fine, transfer_coarse, couple_coarse,
    moments_out, near,
    near_list, far_fine, far_coarse, xs, nb, sb, tf, cf, tc, cc,
    eb, eu, s4, c512, c256, c128, c64, n64, n32, c16, c8, c4, f64,
    g512, g256, g128, g64, g32,
    se, ss, re64, re32, re16, re8, rs64, rs32, rs16, rs8, rs4,
    load_sem, tab_send, tab_recv, halo_send, halo_recv, ring_send, ring_recv,
):
    r = lax.axis_index("rows")
    z = lax.axis_index("rhs")
    k = r // 2
    c = r % 2
    left, right = (r + ROWS - 1) % ROWS, (r + 1) % ROWS
    left2, right2 = (r + ROWS - 2) % ROWS, (r + 2) % ROWS
    partner = r + 1 - 2 * c
    other = (r + ROWS + 2 * c - 1) % ROWS
    z32, z64 = 2 + k // 8, 4 + k // 4

    barrier = pltpu.get_barrier_semaphore()

    def greet_rows(d, carry):
        there = ((k + d) % CHIPS) * 2 + c
        pl.semaphore_signal(barrier, inc=1, device_id={"rows": there}, device_id_type=MESH)
        return carry

    def greet_deep(d, carry):
        pl.semaphore_signal(barrier, inc=1, device_id={"rhs": (z + d) % DEEP}, device_id_type=MESH)
        return carry

    lax.fori_loop(1, DEEP, greet_deep, 0)
    lax.fori_loop(1, CHIPS, greet_rows, 0)
    for there in (partner, other):
        pl.semaphore_signal(barrier, inc=1, device_id={"rows": there}, device_id_type=MESH)

    loads = []

    def load(src, dst):
        copy = pltpu.make_async_copy(src, dst, load_sem.at[len(loads)])
        copy.start()
        loads.append(copy)
        return copy

    get_tc = load(transfer_coarse, tc)
    get_cc = load(couple_coarse, cc)
    get_far = load(far_coarse_in, far_coarse)
    get_tf = load(transfer_fine, tf)
    get_sb = load(basis, sb)
    chunk = 4 * LEAF
    get_xs = [
        load(sources.at[pl.ds(i * chunk, chunk)], xs.at[pl.ds(LEAF + i * chunk, chunk)]) for i in range(4)
    ]
    get_cf = load(couple_fine, cf)
    get_far_fine = load(far_fine_in, far_fine)
    get_near_list = load(near_list_in, near_list)
    get_nb = load(near_blocks, nb)

    spread = jnp.where(iota((RANK, 128), 1) % RANK == iota((RANK, 128), 0), 1.0, 0.0).astype(BF)
    spread_t = jnp.where(iota((128, RANK), 0) % RANK == iota((128, RANK), 1), 1.0, 0.0).astype(BF)

    get_tc.wait()
    wide_e = dot(tc[...].reshape(LPD * RANK, RANK), spread)
    lane_block = iota((RANK, 128), 1) // RANK
    for group in range(2):
        for odd in range(2):
            total = jnp.zeros((RANK, 128), F32)
            for parent in range(4):
                row = (8 * group + 2 * parent + odd) * RANK
                total = total + jnp.where(lane_block == parent, wide_e[row : row + RANK], 0.0)
            se[group, odd * RANK : (odd + 1) * RANK, :] = total.astype(BF)
    get_cc.wait()
    get_far.wait()
    for quarter in range(4):
        wide_s = dot(cc[4 * quarter : 4 * quarter + 4].reshape(4 * 3 * RANK, RANK), spread)
        first_size = {0: 4, 1: 4, 2: 8, 3: 8}[quarter]
        size = jnp.where(z >= 4, 64, jnp.where(z >= 2, 32, jnp.where(z == 1, 16, first_size)))
        for i in range(4):
            row = 4 * quarter + i
            mine = wide_s[i * 3 * RANK : (i + 1) * 3 * RANK]
            heap = z * LPD + row
            at = heap - size
            base = at - row % 2 - 2
            fars = [far_coarse[slot, heap] for slot in range(3)]
            block = routed(mine, fars, base, size)
            if quarter == 1:
                block = jnp.where(z == 0, mine[:RANK], block)
            ss[row * RANK : (row + 1) * RANK, :] = block.astype(BF)

    get_tf.wait()
    fine_e = tf[...].reshape(28 * RANK, RANK)
    eb[...] = jnp.where(block_mask((896, 128), 64, RANK), dot(fine_e, spread), 0.0).astype(BF)
    eu[...] = jnp.where(block_mask((128, 896), RANK, 64), dot_nt(spread_t, fine_e), 0.0).astype(BF)

    get_sb.wait()
    for i in range(4):
        get_xs[i].wait()
        for leaf in range(4 * i, 4 * i + 4):
            product = dot(sb[leaf], xs[LEAF * (leaf + 1) : LEAF * (leaf + 2), :])
            c512[64 + RANK * leaf : 64 + RANK * (leaf + 1), :] = product.astype(BF)

    pl.semaphore_wait(barrier, DEEP - 1 + CHIPS - 1 + 2)

    def table_copy(kind, src, dst, slot, d):
        return pltpu.make_async_remote_copy(
            src_ref=src, dst_ref=dst, send_sem=tab_send.at[slot, d], recv_sem=tab_recv.at[kind],
            device_id={"rhs": (z + d) % DEEP}, device_id_type=MESH,
        )

    e64_at = se.at[(k % 4) // 2]
    e32_at = se.at[(k % 8) // 4]
    rows64 = pl.ds(((4 * k) % LPD) * RANK, 4 * RANK)
    rows32 = pl.ds(((2 * k) % LPD) * RANK, 2 * RANK)
    rows16 = pl.ds(k * RANK, RANK)
    rows8 = pl.ds((8 + k // 2) * RANK, RANK)
    rows4 = pl.ds((4 + k // 4) * RANK, RANK)
    tables = [
        (z64, [(0, e64_at, re64), (1, ss.at[rows64], rs64)]),
        (z32, [(2, e32_at, re32), (3, ss.at[rows32], rs32)]),
        (1, [(4, se, re16), (5, ss.at[rows16], rs16)]),
        (0, [(6, se.at[1], re8), (7, ss.at[rows8], rs8), (8, ss.at[rows4], rs4)]),
    ]
    def send_table(index, item):
        owner, items = tables[index]
        kind, src, dst = items[item]

        @pl.when(z == owner)
        def _():
            def send(d, carry):
                table_copy(kind, src, dst, item, d).start()
                return carry

            lax.fori_loop(1, DEEP, send, 0)
            dst[...] = src[...]

    send_table(0, 0)
    send_table(1, 0)

    def wait_table(index, item):
        owner, items = tables[index]
        kind, src, dst = items[item]

        @pl.when(z != owner)
        def _():
            table_copy(kind, src, dst, item, 1).wait_recv()

    halos = []

    def swap(src, dst, there):
        index = len(halos)
        copy = pltpu.make_async_remote_copy(
            src_ref=src, dst_ref=dst, send_sem=halo_send.at[index], recv_sem=halo_recv.at[index],
            device_id={"rows": there}, device_id_type=MESH,
        )
        copy.start()
        halos.append(copy)
        return copy

    own = c512[64:576, :]
    c256[64:192, :] = dot(eu[:, 0:256], own[:256]).astype(BF)
    c256[192:320, :] = dot(eu[:, 256:512], own[256:]).astype(BF)
    c128[64:192, :] = dot(eu[:, 512:768], c256[64:320, :]).astype(BF)
    mine64 = dot(eu[:64, 768:896], c128[64:192, :]).astype(BF)
    c64[0] = mine64[:, :HALF]
    c64[1] = mine64[:, HALF:]
    rows_mine = pl.ds(64 + 64 * c, 64)
    rows_theirs = pl.ds(128 - 64 * c, 64)
    to_partner = swap(c64.at[1 - c], n64.at[rows_mine], partner)
    n64[rows_mine, :] = c64[c]

    level_halos = []
    for held, count in ((c128, 4), (c256, 8), (c512, 16)):
        rows = count * RANK
        level_halos.append((
            swap(held.at[pl.ds(64, 64)], held.at[pl.ds(64 + rows, 64)], left),
            swap(held.at[pl.ds(rows, 64)], held.at[pl.ds(0, 64)], right),
        ))
    leaf_left = swap(xs.at[pl.ds(LEAF, LEAF)], xs.at[pl.ds(17 * LEAF, LEAF)], left)
    leaf_right = swap(xs.at[pl.ds(16 * LEAF, LEAF)], xs.at[pl.ds(0, LEAF)], right)
    for index, item in ((2, 0), (3, 0), (0, 1), (1, 1), (2, 1), (3, 1), (3, 2)):
        send_table(index, item)

    get_cf.wait()
    get_far_fine.wait()
    for part in range(7):
        wide_s = dot(cf[4 * part : 4 * part + 4].reshape(4 * 3 * RANK, RANK), spread)
        size, first = ((512, 0), (256, 16), (128, 24))[0 if part < 4 else 1 if part < 6 else 2]
        for i in range(4):
            row = 4 * part + i
            j = r * (size // ROWS) + row - first
            fars = [far_fine[slot, row] for slot in range(3)]
            block = routed(wide_s[i * 3 * RANK : (i + 1) * 3 * RANK], fars, j - row % 2 - 2, size)
            s4[row * RANK : (row + 1) * RANK, :] = block.astype(BF)

    get_near_list.wait()
    get_nb.wait()

    def near_leaf(t, carry):
        blocks = []
        for wanted in (-1, 0, 1):
            target = (r * LPD + t + wanted) & 511
            slot = jnp.where(near_list[2, t] == target, 2, jnp.where(near_list[1, t] == target, 1, 0))
            blocks.append(nb[t, slot])
        rows = xs[pl.ds(pl.multiple_of(t * LEAF, LEAF), 3 * LEAF), :]
        near[pl.ds(pl.multiple_of(t * LEAF, LEAF), LEAF), :] = dot(jnp.concatenate(blocks, axis=1), rows).astype(BF)
        return carry

    def near_leaves(first, count):
        def some(i, carry):
            for u in range(UNROLL):
                near_leaf(first + i * UNROLL + u, 0)
            return carry

        lax.fori_loop(0, count // UNROLL, some, 0)

    near_leaves(1, NEAR_A)

    to_partner.wait_recv()
    halos64 = (
        swap(n64.at[pl.ds(64, 64)], n64.at[pl.ds(192, 64)], left2),
        swap(n64.at[pl.ds(128, 64)], n64.at[pl.ds(0, 64)], right2),
    )
    near_leaves(1 + NEAR_A, NEAR_B)
    wait_table(0, 0)
    children = iota((128, 128), 0) // RANK
    lanes = iota((128, 128), 1) // RANK
    packed = re64[...].astype(F32)
    eb64 = jnp.where(lanes == 2 * (k % 2) + children // 2, jnp.concatenate([packed, packed], axis=0), 0.0).astype(BF)
    up = dot_t(eb64, n64[64:192, :])
    n32[64:128, :] = (up[:64] + up[64:]).astype(BF)
    wait_table(1, 0)
    eb32 = jnp.where(iota((64, 128), 1) // RANK == k % 4, re32[...].astype(F32), 0.0).astype(BF)
    up = dot_t(eb32, n32[64:128, :])
    c16[k] = (up[:32] + up[32:64] + up[64:96] + up[96:]).astype(BF)

    def ring_copy(src_chip, there, d):
        return pltpu.make_async_remote_copy(
            src_ref=c16.at[src_chip], dst_ref=c16.at[src_chip],
            send_sem=ring_send.at[d], recv_sem=ring_recv.at[src_chip],
            device_id={"rows": there * 2 + c}, device_id_type=MESH,
        )

    def ring_start(d, carry):
        ring_copy(k, (k + d) % CHIPS, d).start()
        return carry

    lax.fori_loop(1, CHIPS, ring_start, 0)
    halos32 = (
        swap(n32.at[pl.ds(64, 64)], n32.at[pl.ds(128, 64)], left2),
        swap(n32.at[pl.ds(64, 64)], n32.at[pl.ds(0, 64)], right2),
    )

    for (from_left, from_right), held, count, first, out in (
        (level_halos[0], c128, 4, 24, g128), (level_halos[1], c256, 8, 16, g256), (level_halos[2], c512, 16, 0, g512),
    ):
        from_left.wait_recv()
        from_right.wait_recv()
        for pair in range(count // 2):
            window = jnp.concatenate([held[64 * pair : 64 * pair + 64, :], held[64 * pair + 128 : 64 * pair + 192, :]], axis=0)
            blocks = s4[first * RANK + 64 * pair : first * RANK + 64 * pair + 64, :]
            out[64 * pair : 64 * pair + 64, :] = dot(blocks, window)

    near_leaves(1 + NEAR_A + NEAR_B, 14 - NEAR_A - NEAR_B)
    leaf_left.wait_recv()
    leaf_right.wait_recv()
    near_leaf(0, 0)
    near_leaf(15, 0)

    def couple_chip(copies, held, table, blocks, out, pairs):
        for copy in copies:
            copy.wait_recv()
        wait_table(table, 1)
        for pair in range(pairs):
            window = jnp.concatenate([held[64 * pair : 64 * pair + 64, :], held[64 * pair + 128 : 64 * pair + 192, :]], axis=0)
            out[64 * pair : 64 * pair + 64, :] = dot(blocks[64 * pair : 64 * pair + 64, :], window)

    couple_chip(halos64, n64, 0, rs64, g64, 2)

    for item in range(2):
        wait_table(2, item)
    for item in range(3):
        wait_table(3, item)
    mask8 = iota((256, 128), 1) // RANK == iota((256, 128), 0) // 64
    def eight(block):
        wide = block.astype(F32)
        return jnp.where(mask8, jnp.concatenate([wide] * 4, axis=0), 0.0).astype(BF)

    def own_child(block, odd, parent):
        even_rows, odd_rows = block[:RANK].astype(F32), block[RANK:].astype(F32)
        rows = jnp.where(odd == 1, odd_rows, even_rows)
        return jnp.where(iota((RANK, 128), 1) // RANK == parent, rows, 0.0).astype(BF)

    e16 = [eight(re16[0]), eight(re16[1])]
    e8 = eight(re8[...])
    e16_own = own_child(re16[k // 8], k % 2, (k % 8) // 2)
    e8_own = own_child(re8[...], (k // 2) % 2, k // 4)

    def ring_wait(d, carry):
        ring_copy((k + d) % CHIPS, k, d).wait_recv()
        return carry

    for owner, items in tables:
        @pl.when(z == owner)
        def _(items=items):
            for slot, (kind, src, dst) in enumerate(items):
                def sent(d, carry, kind=kind, src=src, dst=dst, slot=slot):
                    table_copy(kind, src, dst, slot, d).wait_send()
                    return carry
                lax.fori_loop(1, DEEP, sent, 0)

    lax.fori_loop(1, CHIPS, ring_wait, 0)
    p16 = k // 2
    for group in range(2):
        up = dot_t(e16[group], c16[8 * group : 8 * group + 8].reshape(256, HALF)).astype(BF)
        c8[2 * group] = up[:64]
        c8[2 * group + 1] = up[64:]
    p8 = k // 4
    all8 = c8[...].reshape(256, HALF)
    up = dot_t(e8, all8).astype(BF)
    for j in range(4):
        c4[j] = up[RANK * j : RANK * (j + 1)]
    window = jnp.concatenate(
        [c16[pl.ds(2 * ((p16 + 7) % 8), 2)].reshape(64, HALF), c16[pl.ds(2 * ((p16 + 1) % 8), 2)].reshape(64, HALF)], axis=0
    )
    g16 = dot(rs16[...], window)
    g8 = dot(rs8[...], jnp.concatenate([c8[(p8 + 3) % 4], c8[(p8 + 1) % 4]], axis=0))
    f4 = dot(rs4[:, :RANK], c4[(k // 4 + 2) % 4]).astype(BF)
    f8 = (g8 + dot(e8_own, jnp.concatenate([f4] * 4, axis=0))).astype(BF)
    f16 = (g16 + dot(e16_own, jnp.concatenate([f8] * 4, axis=0))).astype(BF)

    couple_chip(halos32, n32, 1, rs32, g32, 1)
    f32_ = (g32[...] + dot(eb32, jnp.concatenate([f16] * 4, axis=0))).astype(BF)
    f64_ = (g64[...] + dot(eb64, jnp.concatenate([f32_] * 2, axis=0))).astype(BF)
    f64[0] = f64_[:64]
    f64[1] = f64_[64:]
    back = swap(f64.at[1 - c], f64.at[2 + c], partner)
    f64[2 + c] = f64[c]

    def ring_sent(d, carry):
        ring_copy(k, (k + d) % CHIPS, d).wait_send()
        return carry

    lax.fori_loop(1, CHIPS, ring_sent, 0)
    for copy in halos:
        copy.wait_send()
    back.wait_recv()
    parents = jnp.concatenate([f64[2], f64[3]], axis=1)
    f128 = (g128[...] + dot(eb[768:896, :64], parents)).astype(BF)
    f256 = (g256[...] + dot(eb[512:768, :], f128)).astype(BF)
    for group in range(2):
        rows = slice(256 * group, 256 * group + 256)
        moments_out[rows, :] = (g512[rows, :] + dot(eb[rows, :], f256[128 * group : 128 * group + 128])).astype(BF)


def tree(near_list, far_fine, far_coarse, sources, near_blocks, basis, transfer_fine, couple_fine, transfer_coarse, couple_coarse):
    hbm = pl.BlockSpec(memory_space=pl.ANY)
    vmem = pl.BlockSpec(memory_space=pltpu.VMEM)
    V = pltpu.VMEM
    dma = pltpu.SemaphoreType.DMA
    S = pltpu.SMEM
    scratch = [
        S((3, 16), jnp.int32), S((3, 28), jnp.int32), S((3, 128), jnp.int32),
        V((18 * LEAF, WIDE), BF), V((16, 3, LEAF, LEAF), BF), V((16, RANK, LEAF), BF), V((28, RANK, RANK), BF),
        V((28, 3, RANK, RANK), BF), V((16, RANK, RANK), BF), V((16, 3, RANK, RANK), BF),
        V((896, 128), BF), V((128, 896), BF), V((896, 128), BF),
        V((640, WIDE), BF), V((384, WIDE), BF), V((256, WIDE), BF), V((2, 64, HALF), BF),
        V((256, HALF), BF), V((192, HALF), BF), V((16, RANK, HALF), BF), V((4, 64, HALF), BF), V((4, RANK, HALF), BF),
        V((4, 64, HALF), BF),
        V((512, WIDE), F32), V((256, WIDE), F32), V((128, WIDE), F32), V((128, HALF), F32), V((64, HALF), F32),
        V((2, 64, 128), BF), V((512, 128), BF), V((64, 128), BF), V((64, 128), BF), V((2, 64, 128), BF), V((64, 128), BF),
        V((128, 128), BF), V((64, 128), BF), V((32, 128), BF), V((32, 128), BF), V((32, 128), BF),
        dma((16,)), dma((3, DEEP)), dma((9,)), dma((14,)), dma((14,)), dma((CHIPS,)), dma((CHIPS,)),
    ]
    return pl.pallas_call(
        tree_kernel,
        name="tree",
        out_shape=(jax.ShapeDtypeStruct((512, WIDE), BF), jax.ShapeDtypeStruct((4096, WIDE), BF)),
        in_specs=[hbm] * 10,
        out_specs=(vmem, vmem),
        scratch_shapes=scratch,
        compiler_params=pltpu.CompilerParams(
            collective_id=0, has_side_effects=True, vmem_limit_bytes=TREE_VMEM
        ),
    )(*(pltpu.with_memory_space_constraint(x, pltpu.HBM) for x in (
        near_list, far_fine, far_coarse, sources, near_blocks, basis, transfer_fine, couple_fine, transfer_coarse, couple_coarse
    )))


def join_kernel(near, basis, moments, out, held, out_sem):
    copies = []
    for t in range(LPD):
        rows = pl.ds(LEAF * t, LEAF)
        far = dot_t(basis[t], moments[RANK * t : RANK * (t + 1), :])
        held[rows, :] = (near[rows, :].astype(F32) + far).astype(BF)
        if t % 2:
            both = pl.ds(LEAF * (t - 1), 2 * LEAF)
            copy = pltpu.make_async_copy(held.at[both], out.at[both], out_sem.at[t // 2])
            copy.start()
            copies.append(copy)
    for copy in copies:
        copy.wait()


def join(near, basis, moments):
    vmem = pl.BlockSpec(memory_space=pltpu.VMEM)
    hbm = pl.BlockSpec(memory_space=pl.ANY)
    dma = pltpu.SemaphoreType.DMA
    return pl.pallas_call(
        join_kernel,
        name="join",
        out_shape=jax.ShapeDtypeStruct((4096, WIDE), BF),
        in_specs=[vmem, vmem, vmem],
        out_specs=hbm,
        scratch_shapes=[pltpu.VMEM((4096, WIDE), BF), dma((8,))],
        compiler_params=pltpu.CompilerParams(vmem_limit_bytes=16 * 1024 * 1024),
    )(near, basis, moments)


def body(
    sources, near_blocks, near_list, source_basis, target_basis, transfer_fine, transfer_coarse,
    couple_fine, couple_coarse, far_fine, far_coarse,
):
    moments, near = tree(
        near_list.T, far_fine.T, far_coarse.T, sources, near_blocks, jnp.swapaxes(source_basis, 1, 2),
        transfer_fine, couple_fine, transfer_coarse, couple_coarse,
    )
    return join(near, jnp.swapaxes(target_basis, 1, 2), moments)


def solution(mesh):
    in_specs = (
        P("rows", "rhs"), P("rows", None, None, None), P("rows", None), P("rows", None, None), P("rows", None, None),
        P("rows", None, None), P("rhs", None, None), P("rows", None, None, None), P("rhs", None, None, None),
        P("rows", None), P(),
    )
    return jax.shard_map(body, mesh=mesh, in_specs=in_specs, out_specs=P("rows", "rhs"), check_vma=False)
```
